32 devices in a mesh: groups: 2 (over y), dp: 4 (over z), rep: 4 (over x, core).
Axes of the slice: x: 2, y: 2, z: 4, core: 2. Of those that a mesh axis runs over, the one named last changes fastest.
Arguments:
- latent_store: bfloat16 [8, 48, 576, 128], P(('groups', 'dp'), 'rep'), parts along dimension 0, may hold values from -6 to 6
- page_rank: int32 [8, 48], P('groups', 'rep'), parts along dimension 0, may hold values from 0 to 3, as said below
- page_index: int32 [8, 48], P('groups', 'rep'), parts along dimension 0, may hold values from 0 to 11, as said below
- lengths: int32 [8, 1], P('groups'), parts along dimension 0, may hold values from 1536 to 6144, as said below
- queries: bfloat16 [16, 36864], P(('groups', 'dp')), parts along dimension 0, may hold values from -250 to 250
- new_latent: bfloat16 [16, 576], P(('groups', 'dp')), parts along dimension 0, may hold values from -4 to 4
- up_value: bfloat16 [64, 512, 128], P('dp'), may hold values from -0.25 to 0.25
- out_proj: bfloat16 [8192, 7168], P('dp', 'rep'), may hold values from -0.0625 to 0.0625
- residual: bfloat16 [16, 7168], P(('groups', 'dp'), 'rep'), parts along dimension 0, may hold values from -11 to 11
- norm_gain: float32 [7168], P('rep'), may hold values from 0.1 to 1.9
- w_gate: bfloat16 [7168, 12288], P('rep', 'dp'), may hold values from -0.0625 to 0.0625
- w_up: bfloat16 [7168, 12288], P('rep', 'dp'), may hold values from -0.0625 to 0.0625
- w_down: bfloat16 [12288, 7168], P('dp', 'rep'), may hold values from -0.0546875 to 0.0546875
Outputs:
- layer_out: bfloat16 [16, 7168], P(('groups', 'dp'), 'rep'), parts along dimension 0
The draws below stay inside these ranges and needn't reach their ends.
There are 2 independent parts, one for each index of `groups`. The reference program is written for one: setup_inputs(seed, part) draws one part's arguments, and reference() takes and returns one part's arrays. A program takes and returns all parts, laid end to end along the dimension named above; an argument that names none is the same for every part. Nothing has to cross between parts.
Inputs may be any that keep to these rules, and one draw needn't show every extreme that they name: page_rank[d, q] is the storage rank holding slot q of rank d, on its device with rep index q // 12; one storage device holds at most 3 slot of one rank, and some holds exactly 3. page_index[d, q] is the slot's page among the 12 pages of its storage device; over all ranks every page of every storage device is named by exactly one slot. `lengths`: some request has exactly 6144 tokens.
All inputs are finite; a program needn't handle non-finite values.
Results may differ from the reference program's by a relative error of at most 0.015.
Values may be sent and summed in bfloat16 or wider, within the bound.
A program may use at most 128 MiB of HBM per device.

```python
import jax
import jax.numpy as jnp
from jax import lax

D = 7168
HEADS = 64
CKV = 512
ROPE = 64
VDIM = 128
FF = 12288
PAGE = 128
STEPS = 2
REQ_DP = 1
PAGES = 48
LAT = 576
ROWS = 8
RANKS = 4
QSLOTS = 48
SLOT_DEV = 12


def permute_rows(source_key, count, length):
    row_keys = jax.random.split(source_key, count)
    return jax.vmap(lambda single: jax.random.permutation(single, length))(row_keys).astype(jnp.int32)


def page_tables(key):
    base_key = jax.random.fold_in(key, 11)
    columns = QSLOTS // SLOT_DEV
    key_list = jax.random.split(base_key, 5)
    outer_perm = permute_rows(key_list[0], columns, RANKS)
    inner_perm = permute_rows(key_list[1], columns, RANKS)
    offset_perm = permute_rows(key_list[2], columns, RANKS)
    virtual_slot = permute_rows(key_list[3], columns * RANKS, SLOT_DEV).reshape(columns, RANKS, SLOT_DEV)
    store_perm = permute_rows(key_list[4], columns * RANKS, SLOT_DEV).reshape(columns, RANKS * SLOT_DEV)
    offset_table = jnp.broadcast_to(offset_perm[:, None, :], (columns, RANKS, RANKS))
    offsets = jnp.take_along_axis(offset_table, virtual_slot % RANKS, axis=2)
    position = (inner_perm[:, :, None] + offsets) % RANKS
    outer_table = jnp.broadcast_to(outer_perm[:, None, :], (columns, RANKS, RANKS))
    source_rank = jnp.take_along_axis(outer_table, position, axis=2)
    store_table = jnp.broadcast_to(store_perm[:, None, :], (columns, RANKS, RANKS * SLOT_DEV))
    store_slot = jnp.take_along_axis(store_table, source_rank * SLOT_DEV + virtual_slot, axis=2)
    rank_table = source_rank.transpose(1, 0, 2).reshape(RANKS, QSLOTS).astype(jnp.int32)
    index_table = store_slot.transpose(1, 0, 2).reshape(RANKS, QSLOTS).astype(jnp.int32)
    return (rank_table, index_table)


def draw_page_rank(key, part):
    return page_tables(key)[0]


def draw_page_index(key, part):
    return page_tables(key)[1]


def draw_lengths(key, part):
    base_key = jax.random.fold_in(key, 31)
    first_key, second_key = jax.random.split(base_key)
    longest = PAGES * PAGE
    drawn = jax.random.randint(first_key, (RANKS * REQ_DP,), longest // 4, longest + 1, dtype=jnp.int32)
    marked = jax.random.randint(second_key, (), 0, RANKS * REQ_DP, dtype=jnp.int32)
    drawn = drawn.at[marked].set(longest)
    return drawn.reshape(RANKS, REQ_DP).astype(jnp.int32)


def latent_rows(key):
    base_key = jax.random.fold_in(key, 47)
    fresh = jax.random.truncated_normal(base_key, -4.0, 4.0, (ROWS // STEPS, STEPS, LAT), jnp.float32)
    return fresh


def draw_new_latent(key, part):
    return latent_rows(key).reshape(ROWS, LAT).astype(jnp.bfloat16)


def draw_queries(key, part):
    fresh = latent_rows(key)
    base_key = jax.random.fold_in(key, 53)
    first_key = jax.random.fold_in(base_key, 0)
    drawn = jax.random.truncated_normal(first_key, -4.0, 4.0, (ROWS // STEPS, STEPS, HEADS, LAT), jnp.float32)
    target = jnp.broadcast_to(fresh[:, :, None, CKV:], (ROWS // STEPS, STEPS, HEADS, ROPE))
    strength = jnp.full((ROWS // STEPS, STEPS, HEADS), 1.6, jnp.float32)
    drawn = drawn.at[..., CKV:].add(strength[..., None] * target)
    return drawn.reshape(ROWS, HEADS * LAT).astype(jnp.bfloat16)


def draw_residual(key, part):
    base_key = jax.random.fold_in(key, 61)
    first_key = jax.random.fold_in(base_key, 0)
    column = jnp.arange(D, dtype=jnp.float32) / D
    values = jax.random.truncated_normal(first_key, -5.0, 5.0, (ROWS, D), jnp.float32) * (1.0 + 0.8 * column)
    return values.astype(jnp.bfloat16)


def shard_levels(stream_key, shape, cuts, smallest, largest):
    gain, own = 1.0, jax.random.fold_in(stream_key, 6)
    for dim, shards_of in cuts:
        steps = jnp.exp(jax.random.uniform(jax.random.fold_in(own, dim), (shards_of,), jnp.float32, smallest / len(cuts), largest / len(cuts)))
        gain = gain * jnp.repeat(steps, shape[dim] // shards_of).reshape([-1 if axis == dim else 1 for axis in range(len(shape))])
    return gain


def gaussian(key, shape, width, bound, pieces=(), kind=jnp.bfloat16):
    result = jax.random.normal(key, shape, jnp.float32) * width
    if len(pieces) > 0:
        result = shard_levels(key, shape, pieces, -0.22, 0.18) * result
    return jnp.clip(result, min=-bound, max=bound).astype(kind)


def setup_inputs(seed: int = 0, part: int = 0) -> dict:
    seeds = jax.random.split(jax.random.key(seed), 14)
    part_splits = jax.random.split(jax.random.fold_in(seeds[13], part), 14)
    latent_store = gaussian(part_splits[0], (RANKS, QSLOTS, LAT, PAGE), 1.0, 6.0, ((0, 4), (1, 4)))
    page_rank = draw_page_rank(jax.random.fold_in(jax.random.fold_in(seeds[13], part), 71), part)
    page_index = draw_page_index(jax.random.fold_in(jax.random.fold_in(seeds[13], part), 71), part)
    lengths = draw_lengths(jax.random.fold_in(jax.random.fold_in(seeds[13], part), 71), part)
    queries = draw_queries(jax.random.fold_in(jax.random.fold_in(seeds[13], part), 71), part)
    new_latent = draw_new_latent(jax.random.fold_in(jax.random.fold_in(seeds[13], part), 71), part)
    up_value = gaussian(seeds[6], (HEADS, CKV, VDIM), CKV ** -0.5, 0.25, ((0, 4),))
    out_proj = gaussian(seeds[7], (HEADS * VDIM, D), (HEADS * VDIM) ** -0.5, 0.0625, ((0, 4), (1, 4)))
    residual = draw_residual(jax.random.fold_in(jax.random.fold_in(seeds[13], part), 71), part)
    norm_gain = jnp.clip(1.0 + 0.18 * jax.random.normal(seeds[9], (D,), jnp.float32), 0.1, 1.9)
    w_gate = gaussian(seeds[10], (D, FF), D ** -0.5, 0.0625, ((0, 4), (1, 4)))
    w_up = gaussian(seeds[11], (D, FF), D ** -0.5, 0.0625, ((0, 4), (1, 4)))
    w_down = gaussian(seeds[12], (FF, D), FF ** -0.5, 0.0546875, ((0, 4), (1, 4)))
    return {"latent_store": latent_store, "page_rank": page_rank, "page_index": page_index, "lengths": lengths, "queries": queries, "new_latent": new_latent, "up_value": up_value, "out_proj": out_proj, "residual": residual, "norm_gain": norm_gain, "w_gate": w_gate, "w_up": w_up, "w_down": w_down}


score_scale = 1.0 / 192.0 ** 0.5
epsilon = 1e-06
mask_value = -1e+30

def reference(latent_store, page_rank, page_index, lengths, queries, new_latent, up_value, out_proj, residual, norm_gain, w_gate, w_up, w_down):
    slot_ids = jnp.arange(QSLOTS, dtype=jnp.int32)
    store_base = (slot_ids // SLOT_DEV * SLOT_DEV).astype(jnp.int32)
    query_all = queries.reshape(RANKS, REQ_DP, STEPS, HEADS, LAT)
    fresh_all = new_latent.reshape(RANKS, REQ_DP, STEPS, LAT)

    def one_rank(inputs):
        rank_row, index_row, length_row, query_rank, fresh_rank = inputs
        pages = latent_store[rank_row.astype(jnp.int32), store_base + index_row.astype(jnp.int32)]
        context = pages.reshape(REQ_DP, PAGES, LAT, PAGE).transpose(0, 2, 1, 3).reshape(REQ_DP, LAT, PAGES * PAGE).astype(jnp.float32)
        query_f = query_rank.astype(jnp.float32)
        fresh_f = fresh_rank.astype(jnp.float32)
        context_scores = jnp.einsum('jshl,jlt->jsht', query_f, context) * score_scale
        positions = jnp.arange(PAGES * PAGE, dtype=jnp.int32)
        seen = (positions[None, :] < length_row[:, None])[:, None, None, :]
        context_scores = jnp.where(seen, context_scores, mask_value)
        fresh_scores = jnp.einsum('jshl,jul->jshu', query_f, fresh_f) * score_scale
        step_ids = jnp.arange(STEPS, dtype=jnp.int32)
        fresh_seen = (step_ids[None, :] <= step_ids[:, None])[None, :, None, :]
        fresh_scores = jnp.where(fresh_seen, fresh_scores, mask_value)
        highest = jnp.maximum(lax.optimization_barrier(jnp.max(context_scores, axis=3)), lax.optimization_barrier(jnp.max(fresh_scores, axis=3)))
        context_weights = jnp.where(seen, jnp.exp(context_scores - highest[..., None]), 0.0)
        fresh_weights = jnp.where(fresh_seen, jnp.exp(fresh_scores - highest[..., None]), 0.0)
        denominator = lax.optimization_barrier(jnp.sum(context_weights, axis=3)) + lax.optimization_barrier(jnp.sum(fresh_weights, axis=3))
        context_rounded = lax.optimization_barrier(context_weights.astype(jnp.bfloat16)).astype(jnp.float32)
        fresh_rounded = lax.optimization_barrier(fresh_weights.astype(jnp.bfloat16)).astype(jnp.float32)
        combined = jnp.einsum('jsht,jct->jshc', context_rounded, context[:, :CKV, :])
        combined = combined + jnp.einsum('jshu,juc->jshc', fresh_rounded, fresh_f[:, :, :CKV])
        return (combined / denominator[..., None]).astype(jnp.bfloat16)
    attention = lax.map(one_rank, (page_rank, page_index, lengths, query_all, fresh_all))
    attention = attention.reshape(ROWS, HEADS, CKV)
    head_values = jnp.einsum('rhc,hcv->rhv', attention.astype(jnp.float32), up_value.astype(jnp.float32))
    head_values = head_values.astype(jnp.bfloat16).reshape(ROWS, HEADS * VDIM)
    attn_out = jnp.dot(head_values, out_proj, preferred_element_type=jnp.float32)
    mixed = residual.astype(jnp.float32) + attn_out
    squares = lax.optimization_barrier(jnp.mean(mixed * mixed, axis=1, keepdims=True))
    normed = (mixed * lax.rsqrt(squares + epsilon) * norm_gain).astype(jnp.bfloat16)
    gate = jnp.dot(normed, w_gate, preferred_element_type=jnp.float32)
    up_part = jnp.dot(normed, w_up, preferred_element_type=jnp.float32)
    hidden = (jax.nn.silu(gate) * up_part).astype(jnp.bfloat16)
    return (mixed + jnp.dot(hidden, w_down, preferred_element_type=jnp.float32)).astype(jnp.bfloat16)
```

```python
import functools
import math

import jax
import jax.numpy as jnp
from jax import lax
from jax.experimental import pallas as pl
from jax.experimental.pallas import tpu as pltpu
from jax.sharding import PartitionSpec as P

D = 7168
CKV = 512
PAGE = 128
PAGES = 48


score_scale = 1.0 / math.sqrt(192.0)
epsilon = 1e-06
mask_value = -1e30


def merged_2(array, axis, join):
    gathered = jax.tree.map(
        lambda a, kind: lax.all_gather(a.astype(kind), axis),
        array,
        jax.tree.map(lambda a: jnp.bfloat16 if a.dtype == jnp.float32 else a.dtype, array),
    )

    def take(source):
        return jax.tree.map(
            lambda a, own: lax.dynamic_index_in_dim(a, source, 0, False).astype(own.dtype),
            gathered,
            array,
        )

    return lax.fori_loop(
        1, lax.axis_size(axis), lambda source, state: join(state, take(source)), take(0)
    )


def page_partials(page_keys, page_queries, key_counts):
    scores = (
        jnp.einsum("pshl,plt->psht", page_queries, page_keys, preferred_element_type=jnp.float32)
        * score_scale
    )
    places = lax.broadcasted_iota(jnp.int32, scores.shape, 3)
    visible = places < key_counts[:, None, None, None]
    scores = jnp.where(visible, scores, mask_value)
    row_peak = jnp.max(scores, axis=3)
    weights = jnp.where(visible, jnp.exp(scores - row_peak[..., None]), 0.0)
    row_total = jnp.sum(weights, axis=3)
    partial_value = jnp.einsum(
        "psht,pct->pshc",
        weights.astype(jnp.bfloat16),
        page_keys[:, :CKV, :],
        preferred_element_type=jnp.float32,
    )
    return (partial_value, row_peak, row_total)


def join_pages(partial_value, row_peak, row_total, slot_request, requests):
    owner_mask = slot_request[None, :] == jnp.arange(requests, dtype=jnp.int32)[:, None]
    spread = owner_mask[:, :, None, None]
    best_peak = jnp.max(jnp.where(spread, row_peak[None], mask_value), axis=1)
    factor = jnp.where(spread, jnp.exp(row_peak[None] - best_peak[:, None]), 0.0)
    joined = jnp.einsum("jpsh,pshc->jshc", factor, partial_value, precision=lax.Precision.HIGHEST)
    summed = jnp.sum(factor * row_total[None], axis=1)
    return (joined, best_peak, summed)


def combine(former, latter):
    former_sum, former_peak, former_total = former
    latter_sum, latter_peak, latter_total = latter
    highest = jnp.maximum(former_peak, latter_peak)
    former_scale = jnp.exp(former_peak - highest)
    latter_scale = jnp.exp(latter_peak - highest)
    merged_sum = former_sum * former_scale[..., None] + latter_sum * latter_scale[..., None]
    return (merged_sum, highest, former_total * former_scale + latter_total * latter_scale)


def fresh_partial(query_rows, fresh_rows, active):
    scores = (
        jnp.einsum("jshl,jul->jshu", query_rows, fresh_rows, preferred_element_type=jnp.float32)
        * score_scale
    )
    step_query = lax.broadcasted_iota(jnp.int32, scores.shape, 1)
    step_key = lax.broadcasted_iota(jnp.int32, scores.shape, 3)
    visible = (step_key <= step_query) & active
    scores = jnp.where(visible, scores, mask_value)
    row_peak = jnp.max(scores, axis=3)
    weights = jnp.where(visible, jnp.exp(scores - row_peak[..., None]), 0.0)
    row_total = jnp.sum(weights, axis=3)
    partial_value = jnp.einsum(
        "jshu,juc->jshc",
        weights.astype(jnp.bfloat16),
        fresh_rows[:, :, :CKV],
        preferred_element_type=jnp.float32,
    )
    return (partial_value, row_peak, row_total)


MESH = pl.DeviceIdType.MESH


def tile_of(width):
    for tile in (512, 256, 128):
        if width % tile == 0:
            return tile
    return width


def feed_forward_kernel(
    dp,
    rep,
    headed_ref,
    residual_ref,
    gain_ref,
    up_value_hbm,
    out_proj_hbm,
    w_gate_hbm,
    w_up_hbm,
    w_down_hbm,
    out_ref,
    up_value,
    out_proj,
    w_gate,
    w_up,
    w_down,
    values,
    res_buf,
    op_buf,
    mixed,
    scaled,
    sq_buf,
    gu_buf,
    hidden,
    down_send,
    down_recv,
    weight_sem,
    res_send,
    res_recv,
    op_send,
    op_recv,
    sq_send,
    sq_recv,
    gu_send,
    gu_recv,
    dn_send,
    dn_recv,
):
    my_rank = lax.axis_index("dp")
    my_column = lax.axis_index("rep")
    weights = []
    for i, (source, target) in enumerate(
        (
            (up_value_hbm, up_value),
            (out_proj_hbm, out_proj),
            (w_gate_hbm, w_gate),
            (w_up_hbm, w_up),
            (w_down_hbm, w_down),
        )
    ):
        copy = pltpu.make_async_copy(source, target, weight_sem.at[i])
        copy.start()
        weights.append(copy)

    barrier = pltpu.get_barrier_semaphore()
    ranks = [lax.rem(my_rank + k, dp) for k in range(1, dp)]
    columns = [lax.rem(my_column + k, rep) for k in range(1, rep)]
    for peer in ranks:
        pl.semaphore_signal(barrier, inc=1, device_id={"dp": peer}, device_id_type=MESH)
    for peer in columns:
        pl.semaphore_signal(barrier, inc=1, device_id={"rep": peer}, device_id_type=MESH)
    pl.semaphore_wait(barrier, dp - 1 + rep - 1)

    def to(axis, peer, source, target, send, recv):
        return pltpu.make_async_remote_copy(
            src_ref=source,
            dst_ref=target,
            send_sem=send,
            recv_sem=recv,
            device_id={axis: peer},
            device_id_type=MESH,
        )

    def spread(axis, source, target, send, recv):
        peers = ranks if axis == "dp" else columns
        copies = [
            to(axis, peer, source, target, send.at[k], recv.at[k]) for k, peer in enumerate(peers)
        ]
        for copy in copies:
            copy.start()
        return copies

    res_copies = spread("dp", residual_ref, res_buf.at[my_rank], res_send, res_recv)
    res_buf[my_rank] = residual_ref[...]

    heads, rows, _ = headed_ref.shape
    rows_here, width = residual_ref.shape
    vdim = up_value.shape[2]
    weights[0].wait()
    for h in range(heads):
        values[:, h * vdim : (h + 1) * vdim] = jnp.dot(
            headed_ref[h], up_value[h], preferred_element_type=jnp.float32
        ).astype(jnp.bfloat16)

    weights[1].wait()
    tile = tile_of(width)

    def project(i, carry):
        at = pl.ds(pl.multiple_of(i * tile, tile), tile)
        op_buf[my_rank, :, at] = jnp.dot(
            values[...], out_proj[:, at], preferred_element_type=jnp.float32
        ).astype(jnp.bfloat16)
        return carry

    lax.fori_loop(0, width // tile, project, 0)
    op_copies = spread("dp", op_buf.at[my_rank], op_buf.at[my_rank], op_send, op_recv)
    for copy in res_copies:
        copy.wait()
    for copy in op_copies:
        copy.wait()
    attn_out = op_buf[0].astype(jnp.float32)
    for source in range(1, dp):
        attn_out += op_buf[source].astype(jnp.float32)
    squares = []
    for source in range(dp):
        part = attn_out[source * rows_here : (source + 1) * rows_here]
        mixed[source] = res_buf[source].astype(jnp.float32) + part
    whole = jnp.concatenate([mixed[source] for source in range(dp)], axis=0)
    squares = jnp.sum(whole * whole, axis=1, keepdims=True)
    sq_buf[my_column] = jnp.broadcast_to(squares, (rows, 128))
    sq_copies = spread("rep", sq_buf.at[my_column], sq_buf.at[my_column], sq_send, sq_recv)
    scaled[...] = (whole * gain_ref[...]).astype(jnp.bfloat16)

    chunks, chunk = gu_buf.shape[1], gu_buf.shape[4]
    step = tile_of(chunk)
    weights[2].wait()
    weights[3].wait()
    gu_copies = []
    for c in range(chunks):

        def gate_up(i, carry):
            at = pl.ds(pl.multiple_of(i * step, step), step)
            source = pl.ds(pl.multiple_of(c * chunk + i * step, step), step)
            gu_buf[my_column, c, 0, :, at] = jnp.dot(
                scaled[...], w_gate[:, source], preferred_element_type=jnp.float32
            ).astype(jnp.bfloat16)
            gu_buf[my_column, c, 1, :, at] = jnp.dot(
                scaled[...], w_up[:, source], preferred_element_type=jnp.float32
            ).astype(jnp.bfloat16)
            return carry

        lax.fori_loop(0, chunk // step, gate_up, 0)
        block = gu_buf.at[my_column, c]
        gu_copies.append(spread("rep", block, block, gu_send.at[c], gu_recv.at[c]))

    for copy in sq_copies:
        copy.wait()
    total = sq_buf[0]
    for source in range(1, rep):
        total += sq_buf[source]
    scale = lax.rsqrt(total[:, :1] / D + epsilon)
    for c in range(chunks):
        for copy in gu_copies[c]:
            copy.wait()
        gate = gu_buf[0, c, 0].astype(jnp.float32)
        up = gu_buf[0, c, 1].astype(jnp.float32)
        for source in range(1, rep):
            gate += gu_buf[source, c, 0].astype(jnp.float32)
            up += gu_buf[source, c, 1].astype(jnp.float32)
        gate = gate * scale
        up = up * scale
        hidden[:, c * chunk : (c + 1) * chunk] = (gate / (1.0 + jnp.exp(-gate)) * up).astype(
            jnp.bfloat16
        )

    weights[4].wait()

    def project_down(i, carry):
        at = pl.ds(pl.multiple_of(i * tile, tile), tile)
        part = jnp.dot(hidden[...], w_down[:, at], preferred_element_type=jnp.float32).astype(
            jnp.bfloat16
        )
        for p in range(dp):
            down_send[p, :, at] = part[p * rows_here : (p + 1) * rows_here]
        return carry

    lax.fori_loop(0, width // tile, project_down, 0)
    dn_copies = [
        to("dp", peer, down_send.at[peer], down_recv.at[my_rank], dn_send.at[k], dn_recv.at[k])
        for k, peer in enumerate(ranks)
    ]
    for copy in dn_copies:
        copy.start()
    result = mixed[my_rank] + down_send[my_rank].astype(jnp.float32)
    for copy in dn_copies:
        copy.wait()
    for peer in ranks:
        result += down_recv[peer].astype(jnp.float32)
    out_ref[...] = result.astype(jnp.bfloat16)


def feed_forward(headed, residual, norm_gain, up_value, out_proj, w_gate, w_up, w_down):
    dp, rep = lax.axis_size("dp"), lax.axis_size("rep")
    heads, rows, _ = headed.shape
    rows_here, width = residual.shape
    inner, hidden_width = out_proj.shape[0], w_gate.shape[1]
    chunks = 3 if hidden_width % (3 * 128) == 0 else 1
    bf16, f32 = jnp.bfloat16, jnp.float32
    dma = pltpu.SemaphoreType.DMA
    vmem = pl.BlockSpec(memory_space=pltpu.VMEM)
    hbm = pl.BlockSpec(memory_space=pl.ANY)
    return pl.pallas_call(
        functools.partial(feed_forward_kernel, dp, rep),
        out_shape=jax.ShapeDtypeStruct((rows_here, width), bf16),
        in_specs=[vmem, vmem, vmem] + [hbm] * 5,
        out_specs=vmem,
        scratch_shapes=[
            pltpu.VMEM(up_value.shape, bf16),
            pltpu.VMEM(out_proj.shape, bf16),
            pltpu.VMEM(w_gate.shape, bf16),
            pltpu.VMEM(w_up.shape, bf16),
            pltpu.VMEM(w_down.shape, bf16),
            pltpu.VMEM((rows, inner), bf16),
            pltpu.VMEM((dp, rows_here, width), bf16),
            pltpu.VMEM((dp, rows, width), bf16),
            pltpu.VMEM((dp, rows_here, width), f32),
            pltpu.VMEM((rows, width), bf16),
            pltpu.VMEM((rep, rows, 128), f32),
            pltpu.VMEM((rep, chunks, 2, rows, hidden_width // chunks), bf16),
            pltpu.VMEM((rows, hidden_width), bf16),
            pltpu.VMEM((dp, rows_here, width), bf16),
            pltpu.VMEM((dp, rows_here, width), bf16),
            dma((5,)),
            dma((dp - 1,)),
            dma((dp - 1,)),
            dma((dp - 1,)),
            dma((dp - 1,)),
            dma((rep - 1,)),
            dma((rep - 1,)),
            dma((chunks, rep - 1)),
            dma((chunks, rep - 1)),
            dma((dp - 1,)),
            dma((dp - 1,)),
        ],
        compiler_params=pltpu.CompilerParams(
            collective_id=0, has_side_effects=True, vmem_limit_bytes=60 * 1024 * 1024
        ),
    )(headed, residual, norm_gain.reshape(1, -1), up_value, out_proj, w_gate, w_up, w_down)


def on_device(
    latent_store,
    page_rank,
    page_index,
    lengths,
    queries,
    new_latent,
    up_value,
    out_proj,
    residual,
    norm_gain,
    w_gate,
    w_up,
    w_down,
):
    my_rank = lax.axis_index("dp")
    my_column = lax.axis_index("rep")
    rank_count, slot_count = page_rank.shape
    capacity = (slot_count + rank_count - 1) // rank_count
    requests = lengths.shape[1]
    rows_here = residual.shape[0]
    steps_count = rows_here // requests
    latent_width = new_latent.shape[1]
    head_count = queries.shape[1] // latent_width
    query_rows = queries.reshape(requests, steps_count, head_count, latent_width)
    fresh_rows = new_latent.reshape(requests, steps_count, latent_width)
    slot_order = jnp.arange(slot_count, dtype=jnp.int32)
    request_ids = jnp.arange(requests, dtype=jnp.int32)
    cap_ids = jnp.arange(capacity, dtype=jnp.int32)
    global_slot = my_column * slot_count + slot_order
    slot_request = global_slot // PAGES
    slot_page = global_slot % PAGES
    own_lengths = lax.dynamic_index_in_dim(lengths, my_rank, 0, keepdims=False)
    slot_length = jnp.sum(
        jnp.where(slot_request[:, None] == request_ids[None, :], own_lengths[None, :], 0), axis=1
    )
    key_counts = jnp.clip(slot_length - slot_page * PAGE, 0, PAGE)
    my_sources = lax.dynamic_index_in_dim(page_rank, my_rank, 0, keepdims=False)
    earlier = (my_sources[None, :] == my_sources[:, None]) & (
        slot_order[None, :] < slot_order[:, None]
    )
    arrival_rank = jnp.sum(earlier.astype(jnp.int32), axis=1)
    arrival_slot = my_sources * capacity + arrival_rank
    held_here = page_rank == my_rank
    held_order = jnp.cumsum(held_here.astype(jnp.int32), axis=1) - 1
    selector = held_here[:, None, :] & (held_order[:, None, :] == cap_ids[None, :, None])
    sent_valid = jnp.any(selector, axis=2).reshape(-1)
    sent_page = jnp.sum(jnp.where(selector, page_index[:, None, :], 0), axis=2).reshape(-1)
    stored = latent_store[0]
    outgoing = jnp.take(stored, sent_page, axis=0)
    outgoing = jnp.where(sent_valid[:, None, None], outgoing, jnp.zeros_like(outgoing))
    arrived = lax.all_to_all(outgoing, "dp", split_axis=0, concat_axis=0, tiled=True)
    restored = jnp.take(arrived, arrival_slot, axis=0)
    page_queries = jnp.take(query_rows, slot_request, axis=0)
    partial_value, row_peak, row_total = page_partials(restored, page_queries, key_counts)
    joined = join_pages(partial_value, row_peak, row_total, slot_request, requests)
    local_part = combine(joined, fresh_partial(query_rows, fresh_rows, my_column == 0))
    merged = merged_2(local_part, "rep", combine)
    attention = (
        (merged[0] / merged[2][..., None]).astype(jnp.bfloat16).reshape(rows_here, head_count, CKV)
    )
    headed = lax.all_to_all(attention, "dp", split_axis=1, concat_axis=0, tiled=True)
    return feed_forward(
        headed.transpose(1, 0, 2),
        residual,
        norm_gain,
        up_value,
        out_proj,
        w_gate,
        w_up,
        w_down,
    )


def solution(mesh):
    in_specs = (
        P(("groups", "dp"), "rep", None, None),
        P("groups", "rep"),
        P("groups", "rep"),
        P("groups", None),
        P(("groups", "dp"), None),
        P(("groups", "dp"), None),
        P("dp", None, None),
        P("dp", "rep"),
        P(("groups", "dp"), "rep"),
        P("rep"),
        P("rep", "dp"),
        P("rep", "dp"),
        P("dp", "rep"),
    )
    out_specs = P(("groups", "dp"), "rep")
    return jax.shard_map(
        on_device, mesh=mesh, in_specs=in_specs, out_specs=out_specs, check_vma=False
    )
```

```python
import functools
import math

import jax
import jax.numpy as jnp
from jax import lax
from jax.experimental import pallas as pl
from jax.experimental.pallas import tpu as pltpu
from jax.sharding import PartitionSpec as P

D = 7168
CKV = 512
PAGE = 128
PAGES = 48


score_scale = 1.0 / math.sqrt(192.0)
epsilon = 1e-06
mask_value = -1e30


MESH = pl.DeviceIdType.MESH


def tile_of(width):
    for tile in (512, 256, 128):
        if width % tile == 0:
            return tile
    return width


def layer_kernel(
    dp,
    rep,
    query_ref,
    fresh_ref,
    bias_ref,
    residual_ref,
    gain_ref,
    store_hbm,
    up_value_hbm,
    out_proj_hbm,
    w_gate_hbm,
    w_up_hbm,
    w_down_hbm,
    out_ref,
    pages,
    queries,
    scores,
    part,
    part_stat,
    part_recv,
    stat_recv,
    share,
    share_stat,
    share_recv,
    share_stat_recv,
    value_buf,
    up_value,
    out_proj,
    w_gate,
    w_up,
    w_down,
    values,
    res_buf,
    op_buf,
    mixed,
    scaled,
    sq_buf,
    gu_buf,
    hidden,
    down_send,
    down_recv,
    weight_sem,
    q_send,
    q_recv,
    f_send,
    f_recv,
    p_send,
    p_recv,
    s_send,
    s_recv,
    v_send,
    v_recv,
    res_send,
    res_recv,
    op_send,
    op_recv,
    sq_send,
    sq_recv,
    gu_send,
    gu_recv,
    dn_send,
    dn_recv,
):
    my_rank = lax.axis_index("dp")
    my_column = lax.axis_index("rep")
    weights = []
    for i, (source, target) in enumerate(
        (
            (store_hbm.at[0], pages),
            (up_value_hbm, up_value),
            (out_proj_hbm, out_proj),
            (w_gate_hbm, w_gate),
            (w_up_hbm, w_up),
            (w_down_hbm, w_down),
        )
    ):
        copy = pltpu.make_async_copy(source, target, weight_sem.at[i])
        copy.start()
        weights.append(copy)

    barrier = pltpu.get_barrier_semaphore()
    ranks = [lax.rem(my_rank + k, dp) for k in range(1, dp)]
    columns = [lax.rem(my_column + k, rep) for k in range(1, rep)]
    for peer in ranks:
        pl.semaphore_signal(barrier, inc=1, device_id={"dp": peer}, device_id_type=MESH)
    for peer in columns:
        pl.semaphore_signal(barrier, inc=1, device_id={"rep": peer}, device_id_type=MESH)
    pl.semaphore_wait(barrier, dp - 1 + rep - 1)

    def to(axis, peer, source, target, send, recv):
        return pltpu.make_async_remote_copy(
            src_ref=source,
            dst_ref=target,
            send_sem=send,
            recv_sem=recv,
            device_id={axis: peer},
            device_id_type=MESH,
        )

    def spread(axis, source, target, send, recv):
        peers = ranks if axis == "dp" else columns
        copies = [
            to(axis, peer, source, target, send.at[k], recv.at[k]) for k, peer in enumerate(peers)
        ]
        for copy in copies:
            copy.start()
        return copies

    res_copies = spread("dp", residual_ref, res_buf.at[my_rank], res_send, res_recv)
    res_buf[my_rank] = residual_ref[...]

    q_copies = spread("dp", query_ref.at[my_column], queries.at[my_rank, my_column], q_send, q_recv)
    queries[my_rank] = query_ref[...]
    f_copies = []
    for k, copy in enumerate(q_copies):
        copy.wait()
        block = queries.at[lax.rem(my_rank + dp - 1 - k, dp), my_column]
        f_copies.append(spread("rep", block, block, f_send.at[k], f_recv.at[k]))
    for copies in f_copies:
        for copy in copies:
            copy.wait()

    rows_here, width = residual_ref.shape
    rows = dp * rows_here
    page_count, latent_width, page = pages.shape
    query_count = rep * query_ref.shape[1]
    group = dp // rep
    share_rows = query_count // dp
    weights[0].wait()
    row_ids = lax.broadcasted_iota(jnp.int32, (query_count, 1), 0) % rows_here
    lanes = lax.broadcasted_iota(jnp.int32, (query_count, 128), 1)

    def attend(d, carry):
        query = queries[d].reshape(query_count, latent_width)
        for p in range(page_count + 1):
            keys = pages[p] if p < page_count else fresh_ref[...]
            scores[:, p * page : (p + 1) * page] = jnp.dot(
                query, keys, preferred_element_type=jnp.float32
            )
        bias = bias_ref[d]
        limit = bias[0:1]
        for r in range(1, rows_here):
            limit = jnp.where(row_ids == r, bias[r : r + 1], limit)
        visible = limit > 0.5
        score = jnp.where(visible, scores[...] * score_scale, mask_value)
        peak = jnp.max(score, axis=1, keepdims=True)
        weight = jnp.where(visible, jnp.exp(score - peak), 0.0)
        total = jnp.sum(weight, axis=1, keepdims=True)
        weight = weight.astype(jnp.bfloat16)
        value = jnp.zeros((query_count, CKV), jnp.float32)
        for p in range(page_count + 1):
            keys = pages[p, :CKV] if p < page_count else fresh_ref[:CKV]
            value += lax.dot_general(
                weight[:, p * page : (p + 1) * page],
                keys,
                (((1,), (1,)), ((), ())),
                preferred_element_type=jnp.float32,
            )
        part[d // group, d % group] = value.astype(jnp.bfloat16)
        both = jnp.where(lanes % 2 == 0, peak, total)
        part_stat[d // group, d % group] = both.T[:8]
        return carry

    lax.fori_loop(0, dp, attend, 0)

    p_copies = []
    for k, peer in enumerate(columns):
        for j, (source, target) in enumerate(((part, part_recv), (part_stat, stat_recv))):
            copy = to(
                "rep",
                peer,
                source.at[peer],
                target.at[my_column],
                p_send.at[j, k],
                p_recv.at[j, k],
            )
            copy.start()
            p_copies.append(copy)
    part_recv[my_column] = part[my_column]
    stat_recv[my_column] = part_stat[my_column]
    for copy in p_copies:
        copy.wait()
    for g in range(group):
        peaks, totals = [], []
        for c in range(rep):
            stat = stat_recv[c, g]
            peaks.append(jnp.broadcast_to(stat[0:1], (128, query_count)).T[:, :1])
            totals.append(jnp.broadcast_to(stat[1:2], (128, query_count)).T[:, :1])
        best = functools.reduce(jnp.maximum, peaks)
        value = jnp.zeros((query_count, CKV), jnp.float32)
        total = jnp.zeros((query_count, 1), jnp.float32)
        for c in range(rep):
            factor = jnp.exp(peaks[c] - best)
            value += part_recv[c, g].astype(jnp.float32) * factor
            total += totals[c] * factor
        value = value.astype(jnp.bfloat16)
        both = jnp.where(lanes % 2 == 0, best, total)
        for p in range(dp):
            share[p, g] = value[p * share_rows : (p + 1) * share_rows]
            share_stat[p, g] = both[p * share_rows : (p + 1) * share_rows]

    s_copies = []
    for k, peer in enumerate(ranks):
        for j, (source, target) in enumerate(((share, share_recv), (share_stat, share_stat_recv))):
            copy = to(
                "dp",
                peer,
                source.at[peer],
                target.at[my_rank],
                s_send.at[j, k],
                s_recv.at[j, k],
            )
            copy.start()
            s_copies.append(copy)
    share_recv[my_rank] = share[my_rank]
    share_stat_recv[my_rank] = share_stat[my_rank]
    for copy in s_copies:
        copy.wait()
    heads = up_value.shape[0]
    vdim = up_value.shape[2]
    weights[1].wait()
    for g in range(group):
        best = share_stat_recv[0, g][:, 0:1]
        for p in range(1, dp):
            best = jnp.maximum(best, share_stat_recv[p, g][:, 0:1])
        value = jnp.zeros((share_rows, CKV), jnp.float32)
        total = jnp.zeros((share_rows, 1), jnp.float32)
        for p in range(dp):
            factor = jnp.exp(share_stat_recv[p, g][:, 0:1] - best)
            value += share_recv[p, g].astype(jnp.float32) * factor
            total += share_stat_recv[p, g][:, 1:2] * factor
        latent = (value / total).astype(jnp.bfloat16)
        for h in range(heads):
            value_buf[my_column, g, :, h * vdim : (h + 1) * vdim] = jnp.dot(
                latent[h * rows_here : (h + 1) * rows_here],
                up_value[h],
                preferred_element_type=jnp.float32,
            ).astype(jnp.bfloat16)
    for copy in spread(
        "rep", value_buf.at[my_column], value_buf.at[my_column], v_send, v_recv
    ):
        copy.wait()
    values[...] = jnp.concatenate(
        [value_buf[c, g].astype(jnp.float32) for c in range(rep) for g in range(group)], axis=0
    ).astype(jnp.bfloat16)

    weights[2].wait()
    tile = tile_of(width)

    def project(i, carry):
        at = pl.ds(pl.multiple_of(i * tile, tile), tile)
        op_buf[my_rank, :, at] = jnp.dot(
            values[...], out_proj[:, at], preferred_element_type=jnp.float32
        ).astype(jnp.bfloat16)
        return carry

    lax.fori_loop(0, width // tile, project, 0)
    op_copies = spread("dp", op_buf.at[my_rank], op_buf.at[my_rank], op_send, op_recv)
    for copy in res_copies:
        copy.wait()
    for copy in op_copies:
        copy.wait()
    attn_out = op_buf[0].astype(jnp.float32)
    for source in range(1, dp):
        attn_out += op_buf[source].astype(jnp.float32)
    squares = []
    for source in range(dp):
        part = attn_out[source * rows_here : (source + 1) * rows_here]
        mixed[source] = res_buf[source].astype(jnp.float32) + part
    whole = jnp.concatenate([mixed[source] for source in range(dp)], axis=0)
    squares = jnp.sum(whole * whole, axis=1, keepdims=True)
    sq_buf[my_column] = jnp.broadcast_to(squares, (rows, 128))
    sq_copies = spread("rep", sq_buf.at[my_column], sq_buf.at[my_column], sq_send, sq_recv)
    scaled[...] = (whole * gain_ref[...]).astype(jnp.bfloat16)

    chunks, chunk = gu_buf.shape[1], gu_buf.shape[4]
    step = tile_of(chunk)
    weights[3].wait()
    weights[4].wait()
    gu_copies = []
    for c in range(chunks):

        def gate_up(i, carry):
            at = pl.ds(pl.multiple_of(i * step, step), step)
            source = pl.ds(pl.multiple_of(c * chunk + i * step, step), step)
            gu_buf[my_column, c, 0, :, at] = jnp.dot(
                scaled[...], w_gate[:, source], preferred_element_type=jnp.float32
            ).astype(jnp.bfloat16)
            gu_buf[my_column, c, 1, :, at] = jnp.dot(
                scaled[...], w_up[:, source], preferred_element_type=jnp.float32
            ).astype(jnp.bfloat16)
            return carry

        lax.fori_loop(0, chunk // step, gate_up, 0)
        block = gu_buf.at[my_column, c]
        gu_copies.append(spread("rep", block, block, gu_send.at[c], gu_recv.at[c]))

    for copy in sq_copies:
        copy.wait()
    total = sq_buf[0]
    for source in range(1, rep):
        total += sq_buf[source]
    scale = lax.rsqrt(total[:, :1] / D + epsilon)
    for c in range(chunks):
        for copy in gu_copies[c]:
            copy.wait()
        gate = gu_buf[0, c, 0].astype(jnp.float32)
        up = gu_buf[0, c, 1].astype(jnp.float32)
        for source in range(1, rep):
            gate += gu_buf[source, c, 0].astype(jnp.float32)
            up += gu_buf[source, c, 1].astype(jnp.float32)
        gate = gate * scale
        up = up * scale
        hidden[:, c * chunk : (c + 1) * chunk] = (gate / (1.0 + jnp.exp(-gate)) * up).astype(
            jnp.bfloat16
        )

    weights[5].wait()

    def project_down(i, carry):
        at = pl.ds(pl.multiple_of(i * tile, tile), tile)
        part = jnp.dot(hidden[...], w_down[:, at], preferred_element_type=jnp.float32).astype(
            jnp.bfloat16
        )
        for p in range(dp):
            down_send[p, :, at] = part[p * rows_here : (p + 1) * rows_here]
        return carry

    lax.fori_loop(0, width // tile, project_down, 0)
    dn_copies = [
        to("dp", peer, down_send.at[peer], down_recv.at[my_rank], dn_send.at[k], dn_recv.at[k])
        for k, peer in enumerate(ranks)
    ]
    for copy in dn_copies:
        copy.start()
    result = mixed[my_rank] + down_send[my_rank].astype(jnp.float32)
    for copy in dn_copies:
        copy.wait()
    for peer in ranks:
        result += down_recv[peer].astype(jnp.float32)
    out_ref[...] = result.astype(jnp.bfloat16)


def layer(
    query_rows,
    fresh_page,
    bias,
    residual,
    norm_gain,
    latent_store,
    up_value,
    out_proj,
    w_gate,
    w_up,
    w_down,
):
    dp, rep = lax.axis_size("dp"), lax.axis_size("rep")
    rows_here, width = residual.shape
    rows = dp * rows_here
    inner, hidden_width = out_proj.shape[0], w_gate.shape[1]
    group = dp // rep
    query_count = rep * query_rows.shape[1]
    share_rows = query_count // dp
    chunks = 3 if hidden_width % (3 * 128) == 0 else 1
    bf16, f32 = jnp.bfloat16, jnp.float32
    dma = pltpu.SemaphoreType.DMA
    vmem = pl.BlockSpec(memory_space=pltpu.VMEM)
    hbm = pl.BlockSpec(memory_space=pl.ANY)
    return pl.pallas_call(
        functools.partial(layer_kernel, dp, rep),
        out_shape=jax.ShapeDtypeStruct((rows_here, width), bf16),
        in_specs=[vmem] * 5 + [hbm] * 6,
        out_specs=vmem,
        scratch_shapes=[
            pltpu.VMEM(latent_store.shape[1:], bf16),
            pltpu.VMEM((dp,) + query_rows.shape, bf16),
            pltpu.VMEM((query_count, bias.shape[2]), f32),
            pltpu.VMEM((rep, group, query_count, CKV), bf16),
            pltpu.VMEM((rep, group, 8, query_count), f32),
            pltpu.VMEM((rep, group, query_count, CKV), bf16),
            pltpu.VMEM((rep, group, 8, query_count), f32),
            pltpu.VMEM((dp, group, share_rows, CKV), bf16),
            pltpu.VMEM((dp, group, share_rows, 128), f32),
            pltpu.VMEM((dp, group, share_rows, CKV), bf16),
            pltpu.VMEM((dp, group, share_rows, 128), f32),
            pltpu.VMEM((rep, group, rows_here, inner), bf16),
            pltpu.VMEM(up_value.shape, bf16),
            pltpu.VMEM(out_proj.shape, bf16),
            pltpu.VMEM(w_gate.shape, bf16),
            pltpu.VMEM(w_up.shape, bf16),
            pltpu.VMEM(w_down.shape, bf16),
            pltpu.VMEM((rows, inner), bf16),
            pltpu.VMEM((dp, rows_here, width), bf16),
            pltpu.VMEM((dp, rows, width), bf16),
            pltpu.VMEM((dp, rows_here, width), f32),
            pltpu.VMEM((rows, width), bf16),
            pltpu.VMEM((rep, rows, 128), f32),
            pltpu.VMEM((rep, chunks, 2, rows, hidden_width // chunks), bf16),
            pltpu.VMEM((rows, hidden_width), bf16),
            pltpu.VMEM((dp, rows_here, width), bf16),
            pltpu.VMEM((dp, rows_here, width), bf16),
            dma((6,)),
            dma((dp - 1,)),
            dma((dp - 1,)),
            dma((dp - 1, rep - 1)),
            dma((dp - 1, rep - 1)),
            dma((2, rep - 1)),
            dma((2, rep - 1)),
            dma((2, dp - 1)),
            dma((2, dp - 1)),
            dma((rep - 1,)),
            dma((rep - 1,)),
            dma((dp - 1,)),
            dma((dp - 1,)),
            dma((dp - 1,)),
            dma((dp - 1,)),
            dma((rep - 1,)),
            dma((rep - 1,)),
            dma((chunks, rep - 1)),
            dma((chunks, rep - 1)),
            dma((dp - 1,)),
            dma((dp - 1,)),
        ],
        compiler_params=pltpu.CompilerParams(
            collective_id=0, has_side_effects=True, vmem_limit_bytes=60 * 1024 * 1024
        ),
    )(
        query_rows,
        fresh_page,
        bias,
        residual,
        norm_gain.reshape(1, -1),
        latent_store,
        up_value,
        out_proj,
        w_gate,
        w_up,
        w_down,
    )


def on_device(
    latent_store,
    page_rank,
    page_index,
    lengths,
    queries,
    new_latent,
    up_value,
    out_proj,
    residual,
    norm_gain,
    w_gate,
    w_up,
    w_down,
):
    my_rank = lax.axis_index("dp")
    my_column = lax.axis_index("rep")
    rep = lax.axis_size("rep")
    rank_count, slot_count = page_rank.shape
    page_count = latent_store.shape[1]
    requests = lengths.shape[1]
    rows_here = residual.shape[0]
    steps_count = rows_here // requests
    latent_width = new_latent.shape[1]
    head_count = queries.shape[1] // latent_width
    query_rows = queries.reshape(rows_here, head_count, latent_width).transpose(1, 0, 2)
    query_rows = query_rows.reshape(rep, head_count * rows_here // rep, latent_width)
    fresh_page = jnp.pad(new_latent.T, ((0, 0), (0, PAGE - rows_here)))
    global_slot = my_column * slot_count + jnp.arange(slot_count, dtype=jnp.int32)
    row_ids = jnp.arange(rows_here, dtype=jnp.int32)
    row_request = row_ids // steps_count
    slot_counts = jnp.where(
        (global_slot // PAGES)[None, None, :] == row_request[None, :, None],
        jnp.clip(
            jnp.repeat(lengths, steps_count, axis=1)[:, :, None]
            - (global_slot % PAGES * PAGE)[None, None, :],
            0,
            PAGE,
        ),
        0,
    )
    named = (page_rank == my_rank)[:, :, None] & (
        page_index[:, :, None] == jnp.arange(page_count, dtype=jnp.int32)
    )
    limits = jnp.sum(jnp.where(named[:, None], slot_counts[..., None], 0), axis=2)
    places = jnp.arange(PAGE, dtype=jnp.int32)
    seen = places < limits[..., None]
    fresh_seen = (places[None, :] <= row_ids[:, None]) & (
        places[None, :] // steps_count == row_request[:, None]
    )
    fresh_seen = (
        fresh_seen[None]
        & (jnp.arange(rank_count) == my_rank)[:, None, None]
        & (my_column == 0)
    )
    bias = jnp.concatenate([seen, fresh_seen[:, :, None]], axis=2).astype(jnp.float32)
    bias = bias.reshape(rank_count, rows_here, -1)
    return layer(
        query_rows,
        fresh_page,
        bias,
        residual,
        norm_gain,
        latent_store,
        up_value,
        out_proj,
        w_gate,
        w_up,
        w_down,
    )


def solution(mesh):
    in_specs = (
        P(("groups", "dp"), "rep", None, None),
        P("groups", "rep"),
        P("groups", "rep"),
        P("groups", None),
        P(("groups", "dp"), None),
        P(("groups", "dp"), None),
        P("dp", None, None),
        P("dp", "rep"),
        P(("groups", "dp"), "rep"),
        P("rep"),
        P("rep", "dp"),
        P("rep", "dp"),
        P("dp", "rep"),
    )
    out_specs = P(("groups", "dp"), "rep")
    return jax.shard_map(
        on_device, mesh=mesh, in_specs=in_specs, out_specs=out_specs, check_vma=False
    )
```
